256 devices in a mesh: ep: 128 (over z, x, y), half: 2 (over core).
Axes of the slice: x: 4, y: 4, z: 8, core: 2. Of those that a mesh axis runs over, the one named last changes fastest.
Arguments:
- tokens: bfloat16 [16384, 2048], P('ep', 'half'), may hold values from -6 to 6
- gate_weights: float32 [16384, 8], P('ep'), may hold values from 0.05 to 0.3
- expert_ids: int32 [16384, 8], P('ep'), may hold values from 0 to 127, all different within a row; in each aligned block of 128 rows (0 to 127, 128 to 255, ...) at most 10 rows name the same one
- w_gate: bfloat16 [128, 2048, 768], P('ep', None, 'half'), may hold values from -0.125 to 0.125
- w_up: bfloat16 [128, 2048, 768], P('ep', None, 'half'), may hold values from -0.125 to 0.125
- w_down: bfloat16 [128, 768, 2048], P('ep', 'half'), may hold values from -0.21875 to 0.21875
Outputs:
- mixed: bfloat16 [16384, 2048], P('ep', 'half')
The draws below stay inside these ranges and needn't reach their ends.
Inputs may be any that keep to these rules, and one draw needn't show every extreme that they name: `expert_ids`: each row names 8 different experts. Within the rows of one device (aligned blocks of 128 rows) no expert is named by more than 10 rows, and in every draw some expert is named by exactly 10 rows of some block.
All inputs are finite; a program needn't handle non-finite values.
Results may differ from the reference program's by a relative error of at most 0.0085.
Values may be sent and summed in bfloat16 or wider, within the bound.
A program may use at most 64 MiB of HBM per device.

```python
import math
import jax
import jax.numpy as jnp
import numpy as np
from jax import lax

D = 2048
FF = 768
TOP = 8
TOK_DEV = 128
EXPERTS = 128
TOKENS = 16384
CAP = 10
N_EP = 128


def steps_of(own_key, shape, shards, low, largest):
    factor_of = 1.0
    for axis_at, shards_of in shards:
        steps = jax.random.uniform(jax.random.fold_in(jax.random.fold_in(own_key, 6), axis_at), (shards_of,), jnp.float32, low / len(shards), largest / len(shards))
        factor_of = factor_of * jnp.repeat(jnp.exp(steps), shape[axis_at] // shards_of).reshape((-1,) + (1,) * (len(shape) - 1 - axis_at))
    return factor_of


def deal_out(rng, own, number, rows, amount, top, reach, slope):
    sequence = jax.random.permutation(rng, amount)
    crowded, common = shares(amount, rows * top, reach, slope, True), shares(amount, rows * top, reach, slope, False)
    places = jnp.arange(amount)

    def named(lengths, rotation):
        used = int((lengths > 0).sum())
        fixed = max(1, used // 4)
        passed = fixed + (places - fixed + rotation * (used - fixed)) % max(1, amount - fixed)
        return jnp.zeros((amount,), jnp.int32).at[sequence[jnp.where(places < fixed, places, passed)]].set(jnp.asarray(lengths, jnp.int32))

    lengths = jnp.where(number % 4 == 0, named(crowded, number // 4), named(common, number - number // 4 - 1))
    mixed = jax.random.permutation(jax.random.fold_in(own, 3), amount)
    giver, receiver = mixed[0:amount // 2 * 2:2], mixed[1:amount // 2 * 2:2]
    margin = jnp.minimum(lengths[giver] - 1, reach - lengths[receiver]) // 2
    margin = jnp.where((giver == sequence[0]) | (receiver == sequence[0]) | (lengths[receiver] == 0), 0, jnp.maximum(margin, 0))
    passed = jax.random.randint(jax.random.fold_in(own, 4), (amount // 2,), 0, 1 << 20) % (margin + 1)
    lengths = lengths.at[giver].add(-passed).at[receiver].add(passed)
    items = jnp.searchsorted(jnp.cumsum(lengths), jnp.arange(rows * top), side="right").astype(jnp.int32)
    table = items.reshape(top, rows).T
    table = table[jax.random.permutation(jax.random.fold_in(own, 1), rows)]
    rotation = jax.random.randint(jax.random.fold_in(own, 2), (rows, 1), 0, top)
    return jnp.take_along_axis(table, (jnp.arange(top)[None, :] + rotation) % top, axis=1)


def shares(amount, total, limit, lean, full):
    weights = [(1 << 20) // math.isqrt(rank ** lean) + 1 for rank in range(1, amount + 1)]
    largest = limit if full else min(limit, max(-(-total // amount), total * weights[0] // sum(weights)))
    least = 1 if total - largest >= amount - 1 else 0
    holding, rest = [largest] + [least] * (amount - 1), total - largest - least * (amount - 1)
    while rest > 0:
        candidates = [i for i in range(1, amount) if holding[i] < largest] or [i for i in range(1, amount) if holding[i] < limit]
        pool, remaining = sum([weights[i] for i in candidates]), rest
        for i in candidates:
            more = min(limit - holding[i], max(1, remaining * weights[i] // pool), rest)
            holding[i] = holding[i] + more
            rest = rest - more
    return np.array(holding)


def scatter_about(key, extent, deviation, reach, shards=(), kind=jnp.bfloat16):
    entries = jax.random.normal(key, extent, jnp.float32) * deviation
    if len(shards) > 0:
        entries = steps_of(key, extent, shards, -0.22, 0.18) * entries
    return jnp.clip(entries, min=-reach, max=reach).astype(kind)


def setup_inputs(seed: int = 0) -> dict:
    arg_keys = jax.random.split(jax.random.key(seed), 7)
    tokens = scatter_about(arg_keys[0], (TOKENS, D), 1.0, 6.0, ((0, 128), (1, 2)))
    gate_weights = jnp.clip(0.05 + 0.25 * jax.random.uniform(arg_keys[1], (TOKENS, TOP), jnp.float32) ** steps_of(arg_keys[1], (TOKENS, TOP), ((0, 128),), -0.2, 0.2), 0.05, 0.3)
    expert_ids_keys = jax.random.split(jax.random.fold_in(arg_keys[2], 1), TOKENS // TOK_DEV)
    expert_ids_turns = jax.random.permutation(jax.random.fold_in(arg_keys[2], 3), TOKENS // TOK_DEV)
    expert_ids = jax.vmap(lambda own, number: deal_out(jax.random.fold_in(arg_keys[2], 2), own, number, TOK_DEV, EXPERTS, TOP, CAP, 2))(expert_ids_keys, expert_ids_turns).reshape((TOKENS, TOP))
    w_gate = scatter_about(arg_keys[3], (EXPERTS, D, FF), D ** -0.5, 0.125, ((0, 128), (2, 2)))
    w_up = scatter_about(arg_keys[4], (EXPERTS, D, FF), D ** -0.5, 0.125, ((0, 128), (2, 2)))
    w_down = scatter_about(arg_keys[5], (EXPERTS, FF, D), FF ** -0.5, 0.21875, ((0, 128), (1, 2)))
    return {"tokens": tokens, "gate_weights": gate_weights, "expert_ids": expert_ids, "w_gate": w_gate, "w_up": w_up, "w_down": w_down}


def rank_block(block):
    columns = jnp.arange(EXPERTS, dtype=jnp.int32)
    onehot = (block[:, None] == columns[None, :]).astype(jnp.int32)
    before = jnp.cumsum(onehot, axis=0) - onehot
    return jnp.sum(before * onehot, axis=1).astype(jnp.int32)


def reference(tokens, gate_weights, expert_ids, w_gate, w_up, w_down):
    ids = expert_ids.reshape(N_EP, TOK_DEV * TOP).astype(jnp.int32)
    ranks = lax.map(rank_block, ids)
    slot = (ids * CAP + ranks).astype(jnp.int32)
    source = jnp.arange(N_EP, dtype=jnp.int32)[:, None]
    local_token = (jnp.arange(TOK_DEV * TOP, dtype=jnp.int32) // TOP)[None, :]
    token_table = jnp.zeros((N_EP, EXPERTS * CAP), jnp.int32).at[source, slot].set(source * TOK_DEV + local_token)
    weight_table = jnp.zeros((N_EP, EXPERTS * CAP), jnp.float32).at[source, slot].set(gate_weights.reshape(N_EP, TOK_DEV * TOP))
    filled = jnp.zeros((N_EP, EXPERTS * CAP), jnp.bfloat16).at[source, slot].set(jnp.ones((N_EP, TOK_DEV * TOP), jnp.bfloat16))
    token_table = token_table.reshape(N_EP, EXPERTS, CAP).transpose(1, 0, 2).reshape(EXPERTS, N_EP * CAP)
    weight_table = weight_table.reshape(N_EP, EXPERTS, CAP).transpose(1, 0, 2).reshape(EXPERTS, N_EP * CAP)
    filled = filled.reshape(N_EP, EXPERTS, CAP).transpose(1, 0, 2).reshape(EXPERTS, N_EP * CAP)
    middle = FF // 2

    def expert_step(total, inputs):
        gate_mat, up_mat, down_mat, rows, weights, used = inputs
        slot_rows = tokens[rows] * used[:, None]
        gate = jnp.dot(slot_rows, gate_mat, preferred_element_type=jnp.float32)
        up = jnp.dot(slot_rows, up_mat, preferred_element_type=jnp.float32)
        hidden = (jax.nn.silu(gate) * up).astype(jnp.bfloat16)
        first = jnp.dot(hidden[:, :middle], down_mat[:middle], preferred_element_type=jnp.float32)
        second = jnp.dot(hidden[:, middle:], down_mat[middle:], preferred_element_type=jnp.float32)
        first = lax.optimization_barrier(first.astype(jnp.bfloat16)).astype(jnp.float32)
        second = lax.optimization_barrier(second.astype(jnp.bfloat16)).astype(jnp.float32)
        expert_out = lax.optimization_barrier((first + second).astype(jnp.bfloat16)).astype(jnp.float32)
        total = total.at[rows].add(weights[:, None] * expert_out)
        return total, None

    start = jnp.zeros((TOKENS, D), jnp.float32)
    total, unused = lax.scan(expert_step, start, (w_gate, w_up, w_down, token_table, weight_table, filled))
    return total.astype(jnp.bfloat16)
```

```python
import functools

import jax
import jax.numpy as jnp
from jax import lax
from jax.experimental import pallas as pl
from jax.experimental.pallas import tpu as pltpu
from jax.sharding import PartitionSpec as P

NZ, NX, NY = 8, 4, 4
PLANE = NX * NY
CAP = 10
SLOTS = NZ * CAP
BF = jnp.bfloat16
F32 = jnp.float32
CHUNKS = ((0, 256), (256, 256), (512, 256), (768, 256))


def kernel(
    tokens, meta, w_gate, w_up, w_down, out,
    x_all, meta_all, slot_of, weight_of, pack, comb, packed, rows, w_gu, w_dn, acc, hidden,
    y_out, y_in, part, red_out, red_in,
    meta_s, meta_r, zg_s, zg_r, d_s, d_r, b_s, b_r, zr_s, zr_r, wl, ws, wr,
):
    ep = lax.axis_index("ep")
    h = lax.axis_index("half")
    z = lax.div(ep, PLANE)
    xy = lax.rem(ep, PLANE)
    x = lax.div(xy, NY)
    y = lax.rem(xy, NY)
    up = lax.rem(z + 1, NZ) * PLANE + xy
    down = lax.rem(z + NZ - 1, NZ) * PLANE + xy
    tok, half_width = tokens.shape
    ff_half = w_gate.shape[2]
    ff = 2 * ff_half
    nrow = (PLANE // 2) * SLOTS

    def remote(src, dst, s, r, to_ep, to_h):
        return pltpu.make_async_remote_copy(
            src_ref=src, dst_ref=dst, send_sem=s, recv_sem=r,
            device_id={"ep": to_ep, "half": to_h}, device_id_type=pl.DeviceIdType.MESH,
        )

    barrier = pltpu.get_barrier_semaphore()

    def greet_plane(i, _):
        other = lax.rem(xy * 2 + h + i, 2 * PLANE)
        pl.semaphore_signal(
            barrier, 1,
            device_id={"ep": z * PLANE + lax.div(other, 2), "half": lax.rem(other, 2)},
            device_id_type=pl.DeviceIdType.MESH,
        )
        return 0

    def greet_z(i, _):
        pl.semaphore_signal(
            barrier, 1,
            device_id={"ep": lax.rem(z + i, NZ) * PLANE + xy, "half": h},
            device_id_type=pl.DeviceIdType.MESH,
        )
        return 0

    lax.fori_loop(1, NZ, greet_z, 0)
    lax.fori_loop(1, 2 * PLANE, greet_plane, 0)
    pl.semaphore_wait(barrier, NZ - 1 + 2 * PLANE - 1)

    def meta_copy(i):
        return remote(
            meta, meta_all.at[i], meta_s.at[i], meta_r.at[i],
            lax.rem(z + i, NZ) * PLANE + xy, h,
        )

    def up_len(c):
        return 4 if c % 2 == 0 else 3

    def cols(c):
        return pl.ds(*CHUNKS[c])

    def gather_copy(c, pos, upward, own=False):
        src_pos = pos - 1 if upward else pos + 1
        src = tokens.at[:, cols(c)] if own else x_all.at[src_pos, :, cols(c)]
        return remote(
            src, x_all.at[pos, :, cols(c)], zg_s.at[c, pos], zg_r.at[c, pos],
            up if upward else down, h,
        )

    def gather_start(c):
        gather_copy(c, 1, True, own=True).start()
        gather_copy(c, NZ - 1, False, own=True).start()

    def gather_hop(c, s):
        lu = up_len(c)
        ld = NZ - 1 - lu
        if s <= lu:
            gather_copy(c, s, True, own=s == 1).wait_recv()
            if s < lu:
                gather_copy(c, s + 1, True).start()
        if s <= ld:
            gather_copy(c, NZ - s, False, own=s == 1).wait_recv()
            if s < ld:
                gather_copy(c, NZ - s - 1, False).start()

    def gu_cols(k, half):
        return w_gu.at[:, pl.ds(pl.multiple_of(k * ff + half * ff_half, 128), ff_half)]

    def dn_rows(half):
        return w_dn.at[pl.ds(pl.multiple_of(half * ff_half, 128), ff_half), :]

    def weight_copies():
        mine = [
            pltpu.make_async_copy(w_gate.at[0], gu_cols(0, h), wl.at[0]),
            pltpu.make_async_copy(w_up.at[0], gu_cols(1, h), wl.at[1]),
            pltpu.make_async_copy(w_down.at[0], dn_rows(h), wl.at[2]),
        ]
        sent = [
            remote(w_gate.at[0], gu_cols(0, h), ws.at[0], wr.at[0], ep, 1 - h),
            remote(w_up.at[0], gu_cols(1, h), ws.at[1], wr.at[1], ep, 1 - h),
            remote(w_down.at[0], dn_rows(h), ws.at[2], wr.at[2], ep, 1 - h),
        ]
        return mine, sent

    def build_slots():
        for i in range(1, NZ):
            meta_copy(i).wait_recv()
        ids = jnp.concatenate([meta_all[p, 0:8, :] for p in range(NZ)], axis=1)
        gws = jnp.concatenate([meta_all[p, 8:16, :] for p in range(NZ)], axis=1)
        members, weights = [], []
        for o in range(PLANE):
            ox, oy = o // NY, o % NY
            expert = z * PLANE + lax.rem(x + ox, NX) * NY + lax.rem(y + oy, NY)
            hit = ids == expert.astype(F32)
            members.append(jnp.sum(jnp.where(hit, 1.0, 0.0), axis=0, keepdims=True))
            weights.append(jnp.sum(jnp.where(hit, gws, 0.0), axis=0, keepdims=True))
        member = jnp.concatenate(members, axis=0)
        weight_of[...] = jnp.concatenate(weights, axis=0)
        before = (
            lax.broadcasted_iota(jnp.int32, (tok, tok), 0)
            < lax.broadcasted_iota(jnp.int32, (tok, tok), 1)
        )
        before = jnp.where(before, 1.0, 0.0).astype(BF)
        for p in range(NZ):
            m = member[:, p * tok:(p + 1) * tok]
            rank = jnp.dot(m.astype(BF), before, preferred_element_type=F32)
            slot_of[:, p * tok:(p + 1) * tok] = jnp.where(m > 0.5, rank + float(p * CAP), -1.0)

    def build_pack(first, last):
        r = lax.broadcasted_iota(jnp.int32, (SLOTS, NZ * tok), 0).astype(F32)
        for o in range(first, last):
            here = slot_of[o:o + 1, :] == r
            pack[o * SLOTS:(o + 1) * SLOTS, :] = jnp.where(here, 1.0, 0.0).astype(BF)

    def build_comb(first, last):
        e_row = lax.broadcasted_iota(jnp.int32, (PLANE, 256), 0)
        for q in range(first, last):
            lane = lax.broadcasted_iota(jnp.int32, (PLANE, 256), 1) + q * 256
            low = e_row * SLOTS
            spread = jnp.where((lane >= low) & (lane < low + SLOTS), 1.0, 0.0).astype(BF)
            slots_at = lax.dot_general(
                slot_of[...].astype(BF), spread, (((0,), (0,)), ((), ())),
                preferred_element_type=F32)
            weights_at = lax.dot_general(
                weight_of[...].astype(BF), spread, (((0,), (0,)), ((), ())),
                preferred_element_type=F32)
            r = lax.rem(
                lax.broadcasted_iota(jnp.int32, (1, 256), 1) + q * 256, SLOTS).astype(F32)
            comb[:, q * 256:(q + 1) * 256] = jnp.where(slots_at == r, weights_at, 0.0).astype(BF)

    def dispatch_copy(c, o):
        ox, oy = lax.div(o, NY), lax.rem(o, NY)
        to = z * PLANE + lax.rem(x + ox, NX) * NY + lax.rem(y + oy, NY)
        j = ox * 2 + lax.div(oy, 2)
        return remote(
            packed.at[o, :, cols(c)], rows.at[h, j, :, cols(c)],
            d_s.at[c, o], d_r.at[c, h * 8 + j], to, lax.rem(ox + oy, 2),
        )

    def dispatch(c):
        for g in range(2):
            n = PLANE // 2
            block = jnp.dot(
                pack[g * nrow:(g + 1) * nrow, :],
                x_all[:, :, cols(c)].reshape(NZ * tok, CHUNKS[c][1]),
                preferred_element_type=F32,
            ).astype(BF)
            packed[g * n:(g + 1) * n, :, cols(c)] = block.reshape(n, SLOTS, CHUNKS[c][1])
            start = 1 - h if g == 0 else n

            def send(o, _):
                dispatch_copy(c, o).start()
                return 0

            lax.fori_loop(start, (g + 1) * n, send, 0)
            if g == 0:
                @pl.when(h == 0)
                def _():
                    rows[0, 0, :, cols(c)] = packed[0, :, cols(c)]

    def dispatch_wait(c):
        def wait(i, _):
            remote(
                packed.at[0, :, cols(c)], rows.at[lax.div(i, 8), lax.rem(i, 8), :, cols(c)],
                d_s.at[c, 0], d_r.at[c, i], ep, 1 - h,
            ).wait_recv()
            return 0

        lax.fori_loop(1 - h, PLANE, wait, 0)

    last = len(CHUNKS) - 1

    def expert_in(c):
        start, width = CHUNKS[c]
        if c < last:
            for n in range(0, 2 * ff, 512):
                total = None
                for hs in range(2):
                    left = rows[hs, :, :, cols(c)].reshape(nrow, width)
                    right = w_gu[hs * half_width + start:hs * half_width + start + width, n:n + 512]
                    term = jnp.dot(left, right, preferred_element_type=F32)
                    total = term if total is None else total + term
                acc[:, n:n + 512] = total if c == 0 else acc[:, n:n + 512] + total
        else:
            for n in range(0, ff, 256):
                g, u = acc[:, n:n + 256], acc[:, ff + n:ff + n + 256]
                for hs in range(2):
                    left = rows[hs, :, :, cols(c)].reshape(nrow, width)
                    k = pl.ds(hs * half_width + start, width)
                    g = g + jnp.dot(left, w_gu[k, n:n + 256], preferred_element_type=F32)
                    u = u + jnp.dot(left, w_gu[k, ff + n:ff + n + 256], preferred_element_type=F32)
                hidden[:, n:n + 256] = (g / (1.0 + jnp.exp(-g)) * u).astype(BF)

    def return_copy(c, i):
        hd, j = lax.div(i, 8), lax.rem(i, 8)
        ox = lax.div(j, 2)
        oy = 2 * lax.rem(j, 2) + lax.rem(ox + h, 2)
        to = z * PLANE + lax.rem(x - ox + NX, NX) * NY + lax.rem(y - oy + NY, NY)
        return remote(
            y_out.at[hd, j, :, cols(c)], y_in.at[ox * NY + oy, :, cols(c)],
            b_s.at[c, i], b_r.at[c, ox * NY + oy], to, hd,
        )

    def expert_out(c):
        start, width = CHUNKS[c]
        for hd in range(2):
            block = jnp.dot(
                hidden[...], w_dn[:, hd * half_width + start:hd * half_width + start + width],
                preferred_element_type=F32,
            ).astype(BF)
            y_out[hd, :, :, cols(c)] = block.reshape(PLANE // 2, SLOTS, width)
            start_i = 1 - h if hd == 0 else 8

            def send(i, _):
                return_copy(c, i).start()
                return 0

            lax.fori_loop(start_i, 8 * (hd + 1), send, 0)
            if hd == 0:
                @pl.when(h == 0)
                def _():
                    y_in[0, :, cols(c)] = y_out[0, 0, :, cols(c)]

    def return_wait(c):
        def wait(o, _):
            remote(
                y_out.at[0, 0, :, cols(c)], y_in.at[o, :, cols(c)],
                b_s.at[c, 0], b_r.at[c, o], ep, 1 - h,
            ).wait_recv()
            return 0

        lax.fori_loop(1 - h, PLANE, wait, 0)

    def reduce_copy(c, pos, downward):
        to_pos = pos - 1 if downward else pos + 1
        return remote(
            red_out.at[pos, :, cols(c)], red_in.at[to_pos, :, cols(c)],
            zr_s.at[c, pos], zr_r.at[c, to_pos], down if downward else up, h,
        )

    def combine(c):
        width = CHUNKS[c][1]
        return_wait(c)
        part[:, cols(c)] = jnp.dot(
            comb[...], y_in[:, :, cols(c)].reshape(PLANE * SLOTS, width),
            preferred_element_type=F32)
        a, b = up_len(c), up_len(c) + 1
        for pos, downward in ((a, True), (b, False)):
            red_out[pos, :, cols(c)] = part[pos * tok:(pos + 1) * tok, cols(c)].astype(BF)
            reduce_copy(c, pos, downward).start()

    def reduce_hop(c, s):
        a, b = up_len(c) - (s - 1), up_len(c) + 1 + (s - 1)
        for pos, downward in ((a, True), (b, False)):
            if 1 <= pos <= NZ - 1:
                reduce_copy(c, pos + 1 if downward else pos - 1, downward).wait_recv()
                total = part[pos * tok:(pos + 1) * tok, cols(c)] + red_in[pos, :, cols(c)].astype(F32)
                red_out[pos, :, cols(c)] = total.astype(BF)
                reduce_copy(c, pos, downward).start()

    def finish(c):
        reduce_copy(c, 1, True).wait_recv()
        reduce_copy(c, NZ - 1, False).wait_recv()
        total = part[0:tok, cols(c)] + red_in[0, :, cols(c)].astype(F32)
        total = total + red_in[NZ, :, cols(c)].astype(F32)
        out[:, cols(c)] = total.astype(BF)

    for i in range(1, NZ):
        meta_copy(i).start()
    meta_all[0] = meta[...]
    mine, sent = weight_copies()

    def start_weights():
        for cp in mine:
            cp.start()
        for cp in sent:
            cp.start()

    def wait_weights():
        for cp in mine:
            cp.wait()
        for cp in sent:
            cp.wait_recv()

    events = []
    nc = len(CHUNKS)
    for c in range(nc):
        t0 = 2.0 * c
        events.append((t0, functools.partial(gather_start, c)))
        for s in range(1, 5):
            events.append((t0 + s, functools.partial(gather_hop, c, s)))
        events.append((t0 + 4.3, functools.partial(dispatch, c)))
        events.append((t0 + 7.6, functools.partial(dispatch_wait, c)))
        events.append((t0 + 7.7, functools.partial(expert_in, c)))
    events.append((0.2, start_weights))
    events.append((1.2, build_slots))
    events.append((1.4, functools.partial(build_pack, 0, 4)))
    events.append((2.4, functools.partial(build_pack, 4, 10)))
    events.append((3.4, functools.partial(build_pack, 10, 16)))
    events.append((7.55, wait_weights))
    events.append((10.5, functools.partial(build_comb, 0, 5)))
    x_all[0] = tokens[...]
    for _, event in sorted(events, key=lambda e: e[0]):
        event()
    for c in range(nc):
        expert_out(c)
    events = []
    for c in range(nc):
        t0 = 2.5 * c
        events.append((t0, functools.partial(combine, c)))
        for s in range(2, 5):
            events.append((t0 + s - 1, functools.partial(reduce_hop, c, s)))
        events.append((t0 + 4, functools.partial(finish, c)))
    for _, event in sorted(events, key=lambda e: e[0]):
        event()

    for i in range(1, NZ):
        meta_copy(i).wait_send()
    for cp in sent:
        cp.wait_send()
    for c in range(nc):
        lu = up_len(c)
        for pos in range(1, NZ):
            gather_copy(c, pos, pos <= lu, own=pos in (1, NZ - 1)).wait_send()
            reduce_copy(c, pos, pos <= lu).wait_send()

        def drain(i, _):
            dispatch_copy(c, i).wait_send()
            return_copy(c, i).wait_send()
            return 0

        lax.fori_loop(1 - h, PLANE, drain, 0)


def local(tokens, gate_weights, expert_ids, w_gate, w_up, w_down):
    tok, half_width = tokens.shape
    ff_half = w_gate.shape[2]
    width, ff = 2 * half_width, 2 * ff_half
    nrow = (PLANE // 2) * SLOTS
    nc = len(CHUNKS)
    meta = jnp.concatenate([expert_ids.astype(F32).T, gate_weights.T], axis=0)
    vmem = pl.BlockSpec(memory_space=pltpu.VMEM)
    hbm = pl.BlockSpec(memory_space=pl.ANY)
    dma = pltpu.SemaphoreType.DMA
    return pl.pallas_call(
        kernel,
        name="moe",
        out_shape=jax.ShapeDtypeStruct((tok, half_width), BF),
        in_specs=[vmem, vmem, hbm, hbm, hbm],
        out_specs=vmem,
        scratch_shapes=[
            pltpu.VMEM((NZ, tok, half_width), BF),
            pltpu.VMEM((NZ, 16, tok), F32),
            pltpu.VMEM((PLANE, NZ * tok), F32),
            pltpu.VMEM((PLANE, NZ * tok), F32),
            pltpu.VMEM((PLANE * SLOTS, NZ * tok), BF),
            pltpu.VMEM((NZ * tok, PLANE * SLOTS), BF),
            pltpu.VMEM((PLANE, SLOTS, half_width), BF),
            pltpu.VMEM((2, PLANE // 2, SLOTS, half_width), BF),
            pltpu.VMEM((width, 2 * ff), BF),
            pltpu.VMEM((ff, width), BF),
            pltpu.VMEM((nrow, 2 * ff), F32),
            pltpu.VMEM((nrow, ff), BF),
            pltpu.VMEM((2, PLANE // 2, SLOTS, half_width), BF),
            pltpu.VMEM((PLANE, SLOTS, half_width), BF),
            pltpu.VMEM((NZ * tok, half_width), F32),
            pltpu.VMEM((NZ, tok, half_width), BF),
            pltpu.VMEM((NZ + 1, tok, half_width), BF),
            dma((NZ,)), dma((NZ,)),
            dma((nc, NZ)), dma((nc, NZ)),
            dma((nc, PLANE)), dma((nc, PLANE)),
            dma((nc, PLANE)), dma((nc, PLANE)),
            dma((nc, NZ)), dma((nc, NZ + 1)),
            dma((3,)), dma((3,)), dma((3,)),
        ],
        compiler_params=pltpu.CompilerParams(
            collective_id=0, has_side_effects=True, vmem_limit_bytes=60 * 2**20
        ),
    )(tokens, meta, w_gate, w_up, w_down)


def solution(mesh):
    placed = (
        P("ep", "half"),
        P("ep", None),
        P("ep", None),
        P("ep", None, "half"),
        P("ep", None, "half"),
        P("ep", "half", None),
    )
    return jax.shard_map(
        local, mesh=mesh, in_specs=placed, out_specs=P("ep", "half"), check_vma=False
    )
```
